32 devices in a mesh: gx: 8 (over z, y), gy: 4 (over x, core).
Axes of the slice: x: 2, y: 2, z: 4, core: 2. Of those that a mesh axis runs over, the one named last changes fastest.
Arguments:
- states: bfloat16 [80, 8, 256, 1024], P('gx', None, 'gy'), may hold values from -6 to 6
- obs_pert: bfloat16 [80, 4, 1024], P(None, 'gy', 'gx'), may hold values from -6 to 6
- obs_innov: bfloat16 [4, 1024], P('gy', 'gx'), may hold values from -6 to 6
- obs_cell: int32 [4, 1024], P('gy', 'gx'), may hold values from 0 to 8191
- obs_count: int32 [4, 8], P('gy', 'gx'), may hold values from 16 to 128, as said below
Outputs:
- analysis: bfloat16 [80, 8, 256, 1024], P(None, None, 'gy', 'gx')
The draws below stay inside these ranges and needn't reach their ends.
Inputs may be any that keep to these rules, and one draw needn't show every extreme that they name: `obs_count`: at most 128; some tile has exactly 128. `obs_cell`: slots at or after their tile's count are unused.
All inputs are finite; a program needn't handle non-finite values.
Results may differ from the reference program's by a relative error of at most 0.0057.
Values may be sent and summed in bfloat16 or wider, within the bound.
A program may use at most 128 MiB of HBM per device.

```python
import jax
import jax.numpy as jnp
from jax import lax

K = 80
L = 8
TX = 128
TY = 64
OBS_DEV = 128
NS_ITERS = 4
NX = 1024
NY = 256
TILE_ROWS = 4
TILE_COLS = 8
OBS_COLS = 1024


def draw_obs_count(key, part):
    base = jax.random.randint(key, (TILE_ROWS * TILE_COLS,), OBS_DEV // 8, OBS_DEV + 1)
    spot = jax.random.randint(jax.random.fold_in(key, 7), (), 0, TILE_ROWS * TILE_COLS)
    flat = jnp.where(jnp.arange(TILE_ROWS * TILE_COLS) == spot, OBS_DEV, base)
    return flat.reshape(TILE_ROWS, TILE_COLS).astype(jnp.int32)


def plant(entries, own_key, least, top_value):
    extent = entries.shape
    index_at = [jax.random.randint(jax.random.fold_in(own_key, axis), (), 0, extent[axis]) for axis in range(len(extent))]
    entries = entries.at[tuple(index_at)].set(least)
    longest = extent.index(max(extent))
    index_at[longest] = (index_at[longest] + 1) % extent[longest]
    return entries.at[tuple(index_at)].set(top_value)


def block_levels(rng, extent, split, least, top_value):
    def one(axis_at, parts):
        draws = jax.random.uniform(jax.random.fold_in(jax.random.fold_in(rng, 6), axis_at), (parts,), jnp.float32, least / len(split), top_value / len(split))
        return jnp.repeat(jnp.exp(draws), extent[axis_at] // parts).reshape((-1,) + (1,) * (len(extent) - axis_at - 1))

    factor_of = one(*split[0])
    for cut in split[1:]:
        factor_of = factor_of * one(*cut)
    return factor_of


def noise(rng, extent, scale, most, cuts=(), kind=jnp.bfloat16):
    values = scale * jax.random.normal(rng, extent, jnp.float32)
    if cuts:
        values = values * block_levels(rng, extent, cuts, -0.22, 0.18)
    return jnp.clip(values, -most, most).astype(kind)


def setup_inputs(seed: int = 0) -> dict:
    streams_of = jax.random.split(jax.random.key(seed), 6)
    return {
        "states": noise(streams_of[0], (K, L, NY, NX), 1.0, 6.0, ((0, 8), (2, 4))),
        "obs_pert": noise(streams_of[1], (K, TILE_ROWS, OBS_COLS), 1.0, 6.0, ((1, 4), (2, 8))),
        "obs_innov": noise(streams_of[2], (TILE_ROWS, OBS_COLS), 1.0, 6.0, ((0, 4), (1, 8))),
        "obs_cell": plant(jax.random.randint(streams_of[3], (TILE_ROWS, OBS_COLS), 0, TY * TX), jax.random.fold_in(streams_of[3], 1), 0, (TY * TX) - 1).astype(jnp.int32),
        "obs_count": draw_obs_count(jax.random.fold_in(streams_of[5], 71), 0),
    }


def locality(groups, row_index, col_index, tile_rows, tile_cols):
    slot_count = groups.shape[1] // 9
    width_x = TX * tile_cols
    height_y = TY * tile_rows
    position = lax.broadcasted_iota(jnp.int32, (1, 9 * slot_count), 1)
    row_shift = position // (3 * slot_count) - 1
    col_shift = position // slot_count % 3 - 1
    folded = jnp.logical_and(row_index == tile_rows - 1, row_shift == 1)
    src_row = jnp.where(folded, tile_rows - 1, row_index + row_shift)
    src_col = jnp.where(folded, (tile_cols - 1 - col_index + col_shift) % tile_cols, (col_index + col_shift) % tile_cols)
    local_row = groups[-2:-1].astype(jnp.float32)
    local_col = groups[-1:].astype(jnp.float32)
    obs_y = src_row.astype(jnp.float32) * TY + local_row
    obs_x = src_col.astype(jnp.float32) * TX + local_col
    obs_y = jnp.where(folded, 2.0 * height_y - 1.0 - obs_y, obs_y)
    obs_x = jnp.where(folded, width_x - 1.0 - obs_x, obs_x)
    block_y = (row_index * TY + lax.broadcasted_iota(jnp.int32, (TY, 1), 0)).astype(jnp.float32)
    gap_y = obs_y - block_y
    offset = jnp.mod(obs_x - (col_index * TX).astype(jnp.float32), float(width_x))
    gap_x = jnp.where(offset < TX, 0.0, jnp.minimum(offset - (TX - 1.0), width_x - offset))
    radius = float(TY // 2)
    scaled = jnp.minimum(1.0, (gap_x * gap_x + gap_y * gap_y) / (radius * radius))
    return (1.0 - scaled) * (1.0 - scaled)

def batched(left, right):
    return jnp.einsum('bij,bjk->bik', left, right, precision=lax.Precision.HIGHEST)

def transforms(groups, taper, members):
    rows = groups[:members + 1]
    weighted = (rows.astype(jnp.float32)[None] * taper[:, None, :]).astype(jnp.bfloat16)
    products = jnp.einsum('bks,js->bkj', weighted.astype(jnp.float32), groups[:members].astype(jnp.float32))
    covariance = products[:, :members, :]
    projected = products[:, members, :]
    identity = jnp.eye(members, dtype=jnp.float32)
    system = identity[None] + covariance / (members - 1.0)
    norm_scale = jnp.sqrt(lax.optimization_barrier(jnp.sum(system * system, axis=(1, 2))))[:, None, None]
    iterate = system / norm_scale
    inverse = jnp.broadcast_to(identity, system.shape)
    for sweep in range(NS_ITERS):
        correction = 1.5 * identity[None] - 0.5 * batched(inverse, iterate)
        iterate = batched(iterate, correction)
        inverse = batched(correction, inverse)
    spread_weights = inverse / jnp.sqrt(norm_scale)
    mean_weights = batched(inverse, batched(inverse, projected[:, :, None])) / (norm_scale * (members - 1.0))
    return (spread_weights + mean_weights).astype(jnp.bfloat16)

def analysis_step(tile_states, transform):
    average = lax.optimization_barrier(jnp.mean(tile_states.astype(jnp.float32), axis=0))
    perturb = (tile_states.astype(jnp.float32) - average[None]).astype(jnp.bfloat16)
    mixed_members = jnp.einsum('klrx,rkj->jlrx', perturb.astype(jnp.float32), transform.astype(jnp.float32))
    return (average[None] + mixed_members).astype(jnp.bfloat16)

def reference(states, obs_pert, obs_innov, obs_cell, obs_count):
    tile_rows = TILE_ROWS
    tile_cols = TILE_COLS
    members = K
    filled = jnp.arange(OBS_DEV, dtype=jnp.int32)[None, None, :] < obs_count[:, :, None]
    perturbs = obs_pert.reshape(members, tile_rows, tile_cols, OBS_DEV)
    perturbs = jnp.where(filled[None], perturbs, jnp.zeros_like(perturbs))
    innovation = obs_innov.reshape(tile_rows, tile_cols, OBS_DEV)
    innovation = jnp.where(filled, innovation, jnp.zeros_like(innovation))
    obs_cells = obs_cell.reshape(tile_rows, tile_cols, OBS_DEV)
    packed = jnp.concatenate([perturbs, innovation[None], (obs_cells // TX).astype(jnp.bfloat16)[None], (obs_cells % TX).astype(jnp.bfloat16)[None]], axis=0)

    def one_tile(tile_index):
        row_index = tile_index // tile_cols
        col_index = tile_index % tile_cols
        pieces = []
        for row_shift in (-1, 0, 1):
            for col_shift in (-1, 0, 1):
                present = jnp.bool_(True)
                if row_shift == 1:
                    folded = row_index == tile_rows - 1
                    src_row = jnp.where(folded, tile_rows - 1, row_index + 1)
                    src_col = jnp.where(folded, (tile_cols - 1 - col_index + col_shift) % tile_cols, (col_index + col_shift) % tile_cols)
                elif row_shift == -1:
                    src_row = jnp.maximum(row_index - 1, 0)
                    src_col = (col_index + col_shift) % tile_cols
                    present = row_index > 0
                else:
                    src_row = row_index
                    src_col = (col_index + col_shift) % tile_cols
                neighbour = packed[:, src_row.astype(jnp.int32), src_col.astype(jnp.int32), :]
                pieces.append(jnp.where(present, neighbour, jnp.zeros_like(neighbour)))
        groups = jnp.concatenate(pieces, axis=1)
        taper = locality(groups, row_index, col_index, tile_rows, tile_cols)
        transform = transforms(groups, taper, members)
        tile_states = lax.dynamic_slice(states, (jnp.int32(0), jnp.int32(0), (row_index * TY).astype(jnp.int32), (col_index * TX).astype(jnp.int32)), (members, L, TY, TX))
        return analysis_step(tile_states, transform)
    tiles = lax.map(one_tile, jnp.arange(tile_rows * tile_cols, dtype=jnp.int32))
    tiles = tiles.reshape(tile_rows, tile_cols, members, L, TY, TX)
    return tiles.transpose(2, 3, 0, 4, 1, 5).reshape(members, L, TY * tile_rows, TX * tile_cols)
```

```python
import functools

import jax
import jax.numpy as jnp
from jax import lax
from jax.experimental import pallas as pl
from jax.experimental.pallas import tpu as pltpu
from jax.sharding import PartitionSpec as P

TX = 128
TY = 64
NS_ITERS = 4
GROUP = 8
PACK = 96
PIECES = 8
MESH = pl.DeviceIdType.MESH


def split(value):
    high = value.astype(jnp.bfloat16)
    low = (value - high.astype(jnp.float32)).astype(jnp.bfloat16)
    return high, low


def product(left, right):
    dims = (((2,), (1,)), ((0,), (0,)))

    def one(a, b):
        return lax.dot_general(a, b, dims, preferred_element_type=jnp.float32)

    return one(left[0], right[0]) + (one(left[0], right[1]) + one(left[1], right[0]))


def emit(source, out):
    out[...] = source[...]


def pack(members, perturbs, innovation, cells, count, out):
    slot_count = out.shape[1]
    spot = lax.broadcasted_iota(jnp.int32, (members, slot_count), 1)
    live = perturbs[...].astype(jnp.float32)
    out[0:members, :] = jnp.where(spot < count[0, 0], live, 0.0).astype(jnp.bfloat16)
    rest = PACK - members
    spot = lax.broadcasted_iota(jnp.int32, (rest, slot_count), 1)
    level = lax.broadcasted_iota(jnp.int32, (rest, slot_count), 0)
    fresh = jnp.where(spot < count[0, 0], innovation[...].astype(jnp.float32), 0.0)
    place = cells[...]
    rows = (place // TX).astype(jnp.float32)
    columns = (place % TX).astype(jnp.float32)
    tail = jnp.where(level == 1, rows, jnp.where(level == 2, columns, 0.0))
    out[members:PACK, :] = jnp.where(level == 0, fresh, tail).astype(jnp.bfloat16)


def kernel(
    members, tile_cols, tile_rows,
    states, packed, out,
    held, groups, geometry, weights, spread, mixed, average, staged,
    send_sem, recv_sem, obs_send, obs_recv, fold_send, out_sem,
):
    col = lax.axis_index("gx")
    row = lax.axis_index("gy")
    per = members // tile_cols
    levels = states.shape[1]
    chunks = TY // GROUP

    barrier = pltpu.get_barrier_semaphore()

    def greet(step, carry):
        pl.semaphore_signal(
            barrier, inc=1, device_id=(lax.rem(col + step, tile_cols), row), device_id_type=MESH
        )
        return carry

    lax.fori_loop(1, tile_cols, greet, 0)
    for up in (1, tile_rows - 1):
        for side in (tile_cols - 1, 0, 1):
            pl.semaphore_signal(
                barrier, inc=1,
                device_id=(lax.rem(col + side, tile_cols), lax.rem(row + up, tile_rows)),
                device_id_type=MESH,
            )
    pl.semaphore_wait(barrier, tile_cols - 1 + 6)

    def slot(index):
        return groups.at[:, pl.ds(index * TX, TX)]

    def obs_copy(index, target_col, target_row, sems):
        return pltpu.make_async_remote_copy(
            src_ref=packed, dst_ref=slot(index), send_sem=sems, recv_sem=obs_recv.at[index],
            device_id=(target_col, target_row), device_id_type=MESH,
        )

    def obs_self(index):
        return pltpu.make_async_copy(packed, slot(index), obs_recv.at[index])

    def each_obs(act_remote, act_self):
        for side in (-1, 0, 1):
            target = lax.rem(col - side + tile_cols, tile_cols)
            first = 1 + side

            @pl.when(row < tile_rows - 1)
            def _():
                act_remote(obs_copy(first, target, row + 1, obs_send.at[first]))

            if side != 0:
                act_remote(obs_copy(3 + first, target, row, obs_send.at[3 + first]))

            @pl.when(row > 0)
            def _():
                act_remote(obs_copy(6 + first, target, row - 1, obs_send.at[6 + first]))

            folded = lax.rem(2 * tile_cols - 1 - col + side, tile_cols)

            @pl.when(jnp.logical_and(row == tile_rows - 1, folded != col))
            def _():
                act_remote(obs_copy(6 + first, folded, row, fold_send.at[first]))

            if act_self is not None:
                @pl.when(jnp.logical_and(row == tile_rows - 1, folded == col))
                def _():
                    act_self(obs_self(6 + first))

    each_obs(lambda copy: copy.start(), lambda copy: copy.start())
    obs_self(4).start()

    def state_copy(chunk, owner, target):
        return pltpu.make_async_remote_copy(
            src_ref=states.at[:, :, pl.ds(chunk * GROUP, GROUP), pl.ds(pl.multiple_of(target * TX, TX), TX)],
            dst_ref=held.at[chunk, pl.ds(owner * per, per)],
            send_sem=send_sem.at[chunk, target],
            recv_sem=recv_sem.at[chunk, owner],
            device_id=(target, row), device_id_type=MESH,
        )

    def own_copy(chunk):
        return pltpu.make_async_copy(
            states.at[:, :, pl.ds(chunk * GROUP, GROUP), pl.ds(pl.multiple_of(col * TX, TX), TX)],
            held.at[chunk, pl.ds(col * per, per)],
            recv_sem.at[chunk, col],
        )

    def launch(chunk, carry):
        def one(step, inner):
            state_copy(chunk, col, lax.rem(col + step, tile_cols)).start()
            return inner

        lax.fori_loop(1, tile_cols, one, 0)
        own_copy(chunk).start()
        return carry

    lax.fori_loop(0, chunks, launch, 0)

    obs_self(4).wait()
    for index in (3, 5):
        obs_copy(index, col, row, obs_send.at[index]).wait_recv()

    @pl.when(row > 0)
    def _():
        for index in range(3):
            obs_copy(index, col, row, obs_send.at[index]).wait_recv()

    @pl.when(row == 0)
    def _():
        groups[:, 0:3 * TX] = jnp.zeros((PACK, 3 * TX), jnp.bfloat16)

    for side in (-1, 0, 1):
        index = 7 + side
        folded = lax.rem(2 * tile_cols - 1 - col + side, tile_cols)
        alone = jnp.logical_and(row == tile_rows - 1, folded == col)

        @pl.when(alone)
        def _():
            obs_self(index).wait()

        @pl.when(jnp.logical_not(alone))
        def _():
            obs_copy(index, col, row, obs_send.at[index]).wait_recv()

    slots = 9 * TX
    width_x = TX * tile_cols
    height_y = TY * tile_rows
    position = lax.broadcasted_iota(jnp.int32, (1, slots), 1)
    row_shift = position // (3 * TX) - 1
    col_shift = position // TX % 3 - 1
    at_top = row == tile_rows - 1
    folded = jnp.logical_and(at_top, row_shift == 1)
    src_row = jnp.where(folded, tile_rows - 1, row + row_shift)
    src_col = jnp.where(
        folded,
        (2 * tile_cols - 1 - col + col_shift) % tile_cols,
        (col + col_shift + tile_cols) % tile_cols,
    )
    places = groups[members:PACK, :].astype(jnp.float32)
    local_row = places[1:2]
    local_col = places[2:3]
    obs_y = src_row.astype(jnp.float32) * TY + local_row
    obs_x = src_col.astype(jnp.float32) * TX + local_col
    obs_y = jnp.where(folded, 2.0 * height_y - 1.0 - obs_y, obs_y)
    obs_x = jnp.where(folded, width_x - 1.0 - obs_x, obs_x)
    away = obs_x - (col * TX).astype(jnp.float32)
    offset = jnp.where(away < 0.0, away + width_x, away)
    gap_x = jnp.where(offset < TX, 0.0, jnp.minimum(offset - (TX - 1.0), width_x - offset))
    geometry[0:1, :] = obs_y - (row * TY).astype(jnp.float32)
    geometry[1:2, :] = gap_x * gap_x

    radius = float(TY // 2)

    def transforms(step, carry):
        identity = (
            lax.broadcasted_iota(jnp.int32, (members, members), 0)
            == lax.broadcasted_iota(jnp.int32, (members, members), 1)
        ).astype(jnp.float32)
        systems = []
        projections = []
        scales = []
        for inner in range(GROUP):
            gap_y = geometry[0:1, :] - (step * GROUP + inner).astype(jnp.float32)
            scaled = jnp.minimum(1.0, (geometry[1:2, :] + gap_y * gap_y) / (radius * radius))
            taper = (1.0 - scaled) * (1.0 - scaled)
            weighted = (groups[...].astype(jnp.float32) * taper).astype(jnp.bfloat16)
            products = lax.dot_general(
                weighted, groups[0:members, :], (((1,), (1,)), ((), ())),
                preferred_element_type=jnp.float32,
            )
            system = identity + products[0:members] * (1.0 / (members - 1.0))
            square = jnp.sum(jnp.sum(system * system, axis=1, keepdims=True), axis=0, keepdims=True)
            systems.append(system)
            projections.append(products[members:members + 1])
            scales.append(jnp.sqrt(square))
        system = jnp.stack(systems)
        projected = jnp.stack(projections)
        norm_scale = jnp.stack(scales)
        iterate = system * (1.0 / norm_scale)
        inverse = None
        for sweep in range(NS_ITERS):
            iterate_parts = split(iterate)
            if inverse is None:
                correction = 1.5 * identity[None] - 0.5 * iterate
            else:
                inverse_parts = split(inverse)
                correction = 1.5 * identity[None] - 0.5 * product(inverse_parts, iterate_parts)
            correction_parts = split(correction)
            if sweep < NS_ITERS - 1:
                iterate = product(iterate_parts, correction_parts)
            inverse = correction if inverse is None else product(correction_parts, inverse_parts)
        half = jnp.sum(inverse * projected, axis=2, keepdims=True)
        mean = jnp.sum(inverse * half, axis=1, keepdims=True)
        mean = mean / (norm_scale * (members - 1.0))
        total = inverse * lax.rsqrt(norm_scale) + mean
        weights[pl.ds(step * GROUP, GROUP)] = total.astype(jnp.bfloat16)
        return carry

    lax.fori_loop(0, TY // GROUP, transforms, 0)

    def out_copy(chunk):
        return pltpu.make_async_copy(
            staged.at[lax.rem(chunk, 2)],
            out.at[:, :, pl.ds(chunk * GROUP, GROUP), :],
            out_sem.at[lax.rem(chunk, 2)],
        )

    def analyse(chunk, carry):
        def arrived(step, inner):
            owner = lax.rem(col + step, tile_cols)
            state_copy(chunk, owner, owner).wait_recv()
            return inner

        own_copy(chunk).wait()
        lax.fori_loop(1, tile_cols, arrived, 0)

        for level in range(levels):
            tile = held[chunk, :, level].astype(jnp.float32)
            mean = jnp.sum(tile, axis=0) * (1.0 / members)
            average[level] = mean
            perturb = (tile - mean[None]).astype(jnp.bfloat16).astype(jnp.float32)
            spread[level] = perturb.reshape(members * GROUP, TX)
        for inner in range(GROUP):
            block = jnp.concatenate(
                [
                    spread[level, pl.ds(inner, members, stride=GROUP), :].astype(jnp.bfloat16)
                    for level in range(levels)
                ],
                axis=1,
            )
            moved = jnp.dot(
                weights[chunk * GROUP + inner], block, preferred_element_type=jnp.float32
            )
            for level in range(levels):
                mixed[level, pl.ds(inner, members, stride=GROUP), :] = moved[:, level * TX:(level + 1) * TX]

        @pl.when(chunk >= 2)
        def _():
            out_copy(chunk - 2).wait()

        for level in range(levels):
            total = mixed[level].reshape(members, GROUP, TX) + average[level][None]
            staged[lax.rem(chunk, 2), :, level] = total.astype(jnp.bfloat16)
        out_copy(chunk).start()
        return carry

    lax.fori_loop(0, chunks, analyse, 0)
    out_copy(chunks - 2).wait()
    out_copy(chunks - 1).wait()

    def drain(chunk, carry):
        def one(step, inner):
            state_copy(chunk, col, lax.rem(col + step, tile_cols)).wait_send()
            return inner

        lax.fori_loop(1, tile_cols, one, 0)
        return carry

    lax.fori_loop(0, chunks, drain, 0)
    each_obs(lambda copy: copy.wait_send(), None)


def body(states, obs_pert, obs_innov, obs_cell, obs_count):
    members = obs_pert.shape[0]
    slot_count = obs_pert.shape[2]
    levels = states.shape[1]
    tile_cols = lax.axis_size("gx")
    tile_rows = lax.axis_size("gy")
    packed = pl.pallas_call(
        functools.partial(pack, members),
        out_shape=jax.ShapeDtypeStruct((PACK, slot_count), jnp.bfloat16),
        in_specs=[pl.BlockSpec(memory_space=pltpu.VMEM)] * 3 + [pl.BlockSpec(memory_space=pltpu.SMEM)],
        out_specs=pl.BlockSpec(memory_space=pltpu.VMEM),
    )(obs_pert.reshape(members, slot_count), obs_innov, obs_cell, obs_count)
    chunks = TY // GROUP
    result = pl.pallas_call(
        functools.partial(kernel, members, tile_cols, tile_rows),
        out_shape=jax.ShapeDtypeStruct((members, levels, TY, TX), jnp.bfloat16),
        in_specs=[pl.BlockSpec(memory_space=pltpu.HBM), pl.BlockSpec(memory_space=pltpu.VMEM)],
        out_specs=pl.BlockSpec(memory_space=pl.ANY),
        scratch_shapes=[
            pltpu.VMEM((chunks, members, levels, GROUP, TX), jnp.bfloat16),
            pltpu.VMEM((PACK, 9 * slot_count), jnp.bfloat16),
            pltpu.VMEM((8, 9 * slot_count), jnp.float32),
            pltpu.VMEM((TY, members, members), jnp.bfloat16),
            pltpu.VMEM((levels, members * GROUP, TX), jnp.float32),
            pltpu.VMEM((levels, members * GROUP, TX), jnp.float32),
            pltpu.VMEM((levels, GROUP, TX), jnp.float32),
            pltpu.VMEM((2, members, levels, GROUP, TX), jnp.bfloat16),
            pltpu.SemaphoreType.DMA((chunks, tile_cols)),
            pltpu.SemaphoreType.DMA((chunks, tile_cols)),
            pltpu.SemaphoreType.DMA((9,)),
            pltpu.SemaphoreType.DMA((9,)),
            pltpu.SemaphoreType.DMA((3,)),
            pltpu.SemaphoreType.DMA((2,)),
        ],
        compiler_params=pltpu.CompilerParams(
            collective_id=0, has_side_effects=True, vmem_limit_bytes=56 * 1024 * 1024
        ),
    )(states, packed)
    step = members // PIECES
    block = pl.BlockSpec((step, levels, TY, TX), lambda piece: (piece, 0, 0, 0))
    return pl.pallas_call(
        emit,
        grid=(PIECES,),
        out_shape=jax.ShapeDtypeStruct(result.shape, result.dtype),
        in_specs=[block],
        out_specs=block,
    )(result)


def solution(mesh):
    return jax.shard_map(
        body,
        mesh=mesh,
        in_specs=(
            P("gx", None, "gy", None),
            P(None, "gy", "gx"),
            P("gy", "gx"),
            P("gy", "gx"),
            P("gy", "gx"),
        ),
        out_specs=P(None, None, "gy", "gx"),
        check_vma=False,
    )
```
